16 devices in a mesh: emb: 16 (over z, y, x, core).
Axes of the slice: x: 2, y: 2, z: 2, core: 2. Of those that a mesh axis runs over, the one named last changes fastest.
Arguments:
- tok_ids: int32 [8192], P('emb')
- x_in: bfloat16 [8192, 1024], P('emb')
- d_out: bfloat16 [8192, 1024], P('emb')
- ple_tables: bfloat16 [4, 50304, 1024], P(None, 'emb')
- w_up: bfloat16 [4, 1024, 4096], replicated
- w_down: bfloat16 [4, 4096, 1024], replicated
- w_gate: bfloat16 [4, 1024, 1024], replicated
- w_proj: bfloat16 [4, 1024, 1024], replicated
Outputs:
- output 1: bfloat16 [8192, 1024], P('emb')
- output 2: float32 [4, 50304, 1024], P(None, 'emb')
- output 3: float32 [4, 1024, 4096], replicated
- output 4: float32 [4, 4096, 1024], replicated
- output 5: float32 [4, 1024, 1024], replicated
- output 6: float32 [4, 1024, 1024], replicated
All inputs are finite; a program needn't handle non-finite values.
Results may differ from the reference program's by a relative error of at most 0.0161681.
Values are sent between devices in bfloat16 or wider.
A program may use at most 1.25 GiB of HBM per device.

```python
import math
import jax
import jax.numpy as jnp
from jax import lax

VOCAB_SIZE = 50304
MODEL_DIM = 1024
HIDDEN_DIM = 4096
EMBED_DIM = 1024
LAYERS = 4
TOKENS = 8192
SHARDS = 16

ROWS_DEV = VOCAB_SIZE // SHARDS
TOKENS_PER = TOKENS // SHARDS
CAP_ROWS = TOKENS_PER // 4
ROW_BITS = int(math.log2(ROWS_DEV)) + 1
EPS = 1e-6


def draw_ids(key):
    k_hot, k_off, k_row, k_shift, k_perm = jax.random.split(key, 5)
    hot_owner = jax.random.randint(k_hot, (SHARDS, 1), 0, SHARDS)
    start_off = jax.random.randint(k_off, (SHARDS, 1), 0, SHARDS - 1)
    slot_idx = jnp.arange(TOKENS_PER)[None, :]
    spread_owner = (hot_owner + 1 + (start_off + slot_idx - CAP_ROWS) % (SHARDS - 1)) % SHARDS
    owner_dev = jnp.where(slot_idx < CAP_ROWS, hot_owner, spread_owner)
    raw_rows = jax.random.randint(k_row, (SHARDS, TOKENS_PER), 0, ROWS_DEV)
    shift_bits = jax.random.randint(k_shift, (SHARDS, TOKENS_PER), 0, ROW_BITS + 1)
    local_row = jnp.right_shift(raw_rows, shift_bits)
    id_grid = owner_dev * ROWS_DEV + local_row
    id_grid = jax.random.permutation(k_perm, id_grid, axis=1, independent=True)
    return id_grid.reshape(TOKENS).astype(jnp.int32)


def draw_normal(key, shape, scale):
    return (jax.random.normal(key, shape, jnp.float32) * scale).astype(jnp.bfloat16)


def setup_inputs(seed: int = 0) -> dict:
    key_list = jax.random.split(jax.random.key(seed), 8)
    return {
        "tok_ids": draw_ids(key_list[0]),
        "x_in": draw_normal(key_list[1], (TOKENS, MODEL_DIM), 1.0),
        "d_out": draw_normal(key_list[2], (TOKENS, MODEL_DIM), 1.0),
        "ple_tables": draw_normal(key_list[3], (LAYERS, VOCAB_SIZE, EMBED_DIM), 1.0),
        "w_up": draw_normal(key_list[4], (LAYERS, MODEL_DIM, HIDDEN_DIM), MODEL_DIM ** -0.5),
        "w_down": draw_normal(key_list[5], (LAYERS, HIDDEN_DIM, MODEL_DIM), 0.5 * HIDDEN_DIM ** -0.5),
        "w_gate": draw_normal(key_list[6], (LAYERS, MODEL_DIM, EMBED_DIM), MODEL_DIM ** -0.5),
        "w_proj": draw_normal(key_list[7], (LAYERS, EMBED_DIM, MODEL_DIM), 0.35 * EMBED_DIM ** -0.5),
    }


def gelu_tanh(pre_act):
    return jax.nn.gelu(pre_act, approximate=True)


def gelu_back(pre_act, grad_out):
    _, pull_back = jax.vjp(gelu_tanh, pre_act.astype(jnp.float32))
    return pull_back(grad_out.astype(jnp.float32))[0]


def layer_fwd(x_cur, up_mat, down_mat, gate_mat, proj_mat, emb_rows):
    x_wide = x_cur.astype(jnp.float32)
    inv_rms = lax.rsqrt(jnp.mean(x_wide * x_wide, axis=-1, keepdims=True) + EPS)
    normed = (x_wide * inv_rms).astype(jnp.bfloat16)
    hidden = jnp.dot(normed, up_mat, preferred_element_type=jnp.float32).astype(jnp.bfloat16)
    act_out = gelu_tanh(hidden.astype(jnp.float32)).astype(jnp.bfloat16)
    mlp_out = jnp.dot(act_out, down_mat, preferred_element_type=jnp.float32).astype(jnp.bfloat16)
    gate_pre = jnp.dot(normed, gate_mat, preferred_element_type=jnp.float32).astype(jnp.bfloat16)
    gate_act = gelu_tanh(gate_pre.astype(jnp.float32)).astype(jnp.bfloat16)
    mix_rows = (gate_act.astype(jnp.float32) * emb_rows.astype(jnp.float32)).astype(jnp.bfloat16)
    ple_out = jnp.dot(mix_rows, proj_mat, preferred_element_type=jnp.float32).astype(jnp.bfloat16)
    x_next = (x_wide + mlp_out.astype(jnp.float32) + ple_out.astype(jnp.float32)).astype(jnp.bfloat16)
    return x_next, (x_wide, inv_rms, normed, hidden, act_out, gate_pre, gate_act, mix_rows)


def layer_bwd(d_x, saved, emb_rows, up_mat, down_mat, gate_mat, proj_mat):
    x_wide, inv_rms, normed, hidden, act_out, gate_pre, gate_act, mix_rows = saved
    g_out = d_x.astype(jnp.bfloat16)
    d_act = jnp.dot(g_out, down_mat.T, preferred_element_type=jnp.float32).astype(jnp.bfloat16)
    d_hidden = gelu_back(hidden, d_act).astype(jnp.bfloat16)
    d_mix = jnp.dot(g_out, proj_mat.T, preferred_element_type=jnp.float32).astype(jnp.bfloat16)
    d_rows = gate_act.astype(jnp.float32) * d_mix.astype(jnp.float32)
    d_gate_act = (emb_rows.astype(jnp.float32) * d_mix.astype(jnp.float32)).astype(jnp.bfloat16)
    d_gate_pre = gelu_back(gate_pre, d_gate_act).astype(jnp.bfloat16)
    d_norm = jnp.dot(d_hidden, up_mat.T, preferred_element_type=jnp.float32) + jnp.dot(d_gate_pre, gate_mat.T, preferred_element_type=jnp.float32)
    d_x_new = d_x + inv_rms * d_norm - inv_rms ** 3 * x_wide * jnp.mean(d_norm * x_wide, axis=-1, keepdims=True)
    g_up = jnp.dot(normed.T, d_hidden, preferred_element_type=jnp.float32)
    g_down = jnp.dot(act_out.T, g_out, preferred_element_type=jnp.float32)
    g_gate = jnp.dot(normed.T, d_gate_pre, preferred_element_type=jnp.float32)
    g_proj = jnp.dot(mix_rows.T, g_out, preferred_element_type=jnp.float32)
    return d_x_new, (g_up, g_down, g_gate, g_proj), d_rows


def reference(tok_ids, x_in, d_out, ple_tables, w_up, w_down, w_gate, w_proj):
    weights = (w_up, w_down, w_gate, w_proj)
    ids_blocks = tok_ids.reshape(SHARDS, TOKENS_PER)
    x_blocks = x_in.reshape(SHARDS, TOKENS_PER, MODEL_DIM)
    dy_blocks = d_out.reshape(SHARDS, TOKENS_PER, MODEL_DIM)

    def fwd_step(x_cur, layer_in):
        up_mat, down_mat, gate_mat, proj_mat, emb_rows = layer_in
        return layer_fwd(x_cur, up_mat, down_mat, gate_mat, proj_mat, emb_rows)

    def bwd_step(d_x, layer_in):
        saved, up_mat, down_mat, gate_mat, proj_mat, emb_rows = layer_in
        d_x_new, grads, d_rows = layer_bwd(d_x, saved, emb_rows, up_mat, down_mat, gate_mat, proj_mat)
        return d_x_new, (grads, d_rows)

    def block_step(carry, block_in):
        grad_acc, table_acc = carry
        blk_ids, blk_x, blk_dy = block_in
        rows_all = ple_tables[:, blk_ids, :]
        x_last, saved_all = lax.scan(fwd_step, blk_x, weights + (rows_all,))
        _, (grads, d_rows) = lax.scan(bwd_step, blk_dy.astype(jnp.float32), (saved_all,) + weights + (rows_all,), reverse=True)
        grad_acc = tuple(acc_part + new_part for acc_part, new_part in zip(grad_acc, grads))
        table_acc = table_acc.at[:, blk_ids, :].add(d_rows)
        return (grad_acc, table_acc), x_last

    grad_init = tuple(jnp.zeros(weight_mat.shape, jnp.float32) for weight_mat in weights)
    table_init = jnp.zeros(ple_tables.shape, jnp.float32)
    (grad_acc, table_acc), x_done = lax.scan(block_step, (grad_init, table_init), (ids_blocks, x_blocks, dy_blocks))
    x_out = x_done.reshape(TOKENS, MODEL_DIM)
    return (x_out, table_acc, grad_acc[0], grad_acc[1], grad_acc[2], grad_acc[3])
```

```python
import jax
import jax.numpy as jnp
from jax import lax
from jax.experimental import pallas as pl
from jax.experimental.pallas import tpu as pltpu
from jax.sharding import PartitionSpec as P


EPS = 1e-6
CAP_DIV = 4
CORE, X, Y, Z = 1, 2, 4, 8
GROUP = 4


def gelu_tanh(pre_act):
    return jax.nn.gelu(pre_act, approximate=True)


def gelu_back(pre_act, grad_out):
    _, pull_back = jax.vjp(gelu_tanh, pre_act.astype(jnp.float32))
    return pull_back(grad_out.astype(jnp.float32))[0]


def dot32(spec, a, b):
    return jnp.einsum(spec, a, b, preferred_element_type=jnp.float32)


def layer_fwd(x_cur, up_mat, down_mat, gate_mat, proj_mat, emb_rows):
    x_wide = x_cur.astype(jnp.float32)
    inv_rms = lax.rsqrt(jnp.mean(x_wide * x_wide, axis=-1, keepdims=True) + EPS)
    normed = (x_wide * inv_rms).astype(jnp.bfloat16)
    hidden = dot32("nd,df->nf", normed, up_mat).astype(jnp.bfloat16)
    act_out = gelu_tanh(hidden.astype(jnp.float32)).astype(jnp.bfloat16)
    mlp_out = dot32("nf,fd->nd", act_out, down_mat).astype(jnp.bfloat16)
    gate_pre = dot32("nd,de->ne", normed, gate_mat).astype(jnp.bfloat16)
    gate_act = gelu_tanh(gate_pre.astype(jnp.float32)).astype(jnp.bfloat16)
    mix_rows = (gate_act.astype(jnp.float32) * emb_rows.astype(jnp.float32)).astype(jnp.bfloat16)
    ple_out = dot32("ne,ed->nd", mix_rows, proj_mat).astype(jnp.bfloat16)
    x_next = (x_wide + mlp_out.astype(jnp.float32) + ple_out.astype(jnp.float32)).astype(jnp.bfloat16)
    return x_next, (x_wide, inv_rms, normed, hidden, gate_pre, gate_act)


def layer_bwd(d_x, g_out, saved, emb_rows, up_mat, down_mat, gate_mat, proj_mat, need_dx):
    x_wide, inv_rms, _, hidden, gate_pre, gate_act = saved
    d_mix = dot32("nd,ed->ne", g_out, proj_mat).astype(jnp.bfloat16)
    d_rows = gate_act.astype(jnp.float32) * d_mix.astype(jnp.float32)
    if not need_dx:
        return None, d_rows
    d_act = dot32("nd,fd->nf", g_out, down_mat).astype(jnp.bfloat16)
    d_hidden = gelu_back(hidden, d_act).astype(jnp.bfloat16)
    d_gate_act = (emb_rows.astype(jnp.float32) * d_mix.astype(jnp.float32)).astype(jnp.bfloat16)
    d_gate_pre = gelu_back(gate_pre, d_gate_act).astype(jnp.bfloat16)
    d_norm = dot32("nf,df->nd", d_hidden, up_mat) + dot32("ne,de->nd", d_gate_pre, gate_mat)
    d_x_new = d_x + inv_rms * d_norm - inv_rms ** 3 * x_wide * jnp.mean(d_norm * x_wide, axis=-1, keepdims=True)
    return d_x_new, d_rows


def cost(nbytes):
    return pl.CostEstimate(flops=int(nbytes), bytes_accessed=int(nbytes), transcendentals=0)


def weight_slices(quarter, w_up, w_gate, w_down, w_proj, blocks):
    layers, dim, hid = w_up.shape
    emb = w_gate.shape[2]
    hb, eb = hid // (GROUP * blocks), emb // (GROUP * blocks)

    def body(q_ref, up_ref, down_ref, proj_ref, up_out, down_out, proj_out):
        up_out[...] = up_ref[...]
        down_out[...] = down_ref[...]
        proj_out[...] = proj_ref[...]

    return pl.pallas_call(
        body,
        grid_spec=pltpu.PrefetchScalarGridSpec(
            num_scalar_prefetch=1,
            grid=(layers, blocks),
            in_specs=[
                pl.BlockSpec((1, dim, hb), lambda l, j, q: (l, 0, GROUP * j + q[0])),
                pl.BlockSpec((1, hb, dim), lambda l, j, q: (l, GROUP * j + q[0], 0)),
                pl.BlockSpec((1, eb, dim), lambda l, j, q: (l, GROUP * j + q[0], 0)),
            ],
            out_specs=[
                pl.BlockSpec((1, dim, hb), lambda l, j, q: (l, 0, j)),
                pl.BlockSpec((1, hb, dim), lambda l, j, q: (l, j, 0)),
                pl.BlockSpec((1, eb, dim), lambda l, j, q: (l, j, 0)),
            ],
        ),
        out_shape=[
            jax.ShapeDtypeStruct((layers, dim, hid // GROUP), w_up.dtype),
            jax.ShapeDtypeStruct((layers, hid // GROUP, dim), w_up.dtype),
            jax.ShapeDtypeStruct((layers, emb // GROUP, dim), w_up.dtype),
        ],
        cost_estimate=cost(4 * layers * dim * (2 * hid + emb) // GROUP),
        name="weight_slices",
    )(quarter, w_up, w_down, w_proj)


def blank(shapes):
    return pl.pallas_call(
        lambda *refs: None,
        out_shape=[jax.ShapeDtypeStruct(shape, jnp.float32) for shape in shapes],
        out_specs=[pl.BlockSpec(memory_space=pl.ANY)] * len(shapes),
        name="blank",
    )()


def place_cols(layer, buf, out_main, out_side):
    n, rows, dim = buf.shape
    hb = out_main.shape[2] // n
    eb = rows - hb
    at_once = max(1, 128 // eb)

    def body(buf_ref, main_in, side_in, main_ref, side_ref):
        for j in range(at_once):
            main_ref[0, :, j * hb:(j + 1) * hb] = buf_ref[j, :hb].T
        side = jnp.concatenate([buf_ref[j, hb:] for j in range(at_once)], axis=0)
        side_ref[0] = side.T

    return pl.pallas_call(
        body,
        grid=(n // at_once,),
        in_specs=[
            pl.BlockSpec((at_once, rows, dim), lambda j: (j, 0, 0)),
            pl.BlockSpec(memory_space=pl.ANY),
            pl.BlockSpec(memory_space=pl.ANY),
        ],
        out_specs=[
            pl.BlockSpec((1, dim, at_once * hb), lambda j: (layer, 0, j)),
            pl.BlockSpec((1, dim, at_once * eb), lambda j: (layer, 0, j)),
        ],
        out_shape=[
            jax.ShapeDtypeStruct(out_main.shape, out_main.dtype),
            jax.ShapeDtypeStruct(out_side.shape, out_side.dtype),
        ],
        input_output_aliases={1: 0, 2: 1},
        cost_estimate=cost(8 * n * rows * dim),
        name="place_cols",
    )(buf, out_main, out_side)


def place_rows(layer, buf, out_main, out_side):
    n, rows, dim = buf.shape
    hb = out_main.shape[1] // n
    eb = rows - hb
    at_once = 2

    def body(buf_ref, main_in, side_in, main_ref, side_ref):
        for j in range(at_once):
            main_ref[0, j * hb:(j + 1) * hb] = buf_ref[j, :hb]
            side_ref[0, j * eb:(j + 1) * eb] = buf_ref[j, hb:]

    return pl.pallas_call(
        body,
        grid=(n // at_once,),
        in_specs=[
            pl.BlockSpec((at_once, rows, dim), lambda j: (j, 0, 0)),
            pl.BlockSpec(memory_space=pl.ANY),
            pl.BlockSpec(memory_space=pl.ANY),
        ],
        out_specs=[
            pl.BlockSpec((1, at_once * hb, dim), lambda j: (layer, j, 0)),
            pl.BlockSpec((1, at_once * eb, dim), lambda j: (layer, j, 0)),
        ],
        out_shape=[
            jax.ShapeDtypeStruct(out_main.shape, out_main.dtype),
            jax.ShapeDtypeStruct(out_side.shape, out_side.dtype),
        ],
        input_output_aliases={1: 0, 2: 1},
        cost_estimate=cost(8 * n * rows * dim),
        name="place_rows",
    )(buf, out_main, out_side)


def place_table(layer, table, out):
    rows, dim = table.shape
    steps = 3 if rows % 24 == 0 else 1

    def body(table_ref, out_in, out_ref):
        out_ref[0] = table_ref[...]

    return pl.pallas_call(
        body,
        grid=(steps,),
        in_specs=[
            pl.BlockSpec((rows // steps, dim), lambda j: (j, 0)),
            pl.BlockSpec(memory_space=pl.ANY),
        ],
        out_specs=pl.BlockSpec((1, rows // steps, dim), lambda j: (layer, j, 0)),
        out_shape=jax.ShapeDtypeStruct(out.shape, out.dtype),
        input_output_aliases={1: 0},
        cost_estimate=cost(8 * rows * dim),
        name="place_table",
    )(table, out)


def solution(mesh):
    shards = mesh.shape["emb"]

    def swap(arr, axis_bit):
        return lax.ppermute(arr, "emb", [(dev, dev ^ axis_bit) for dev in range(shards)])

    def device_step(tok_ids, x_in, d_out, ple_tables, w_up, w_down, w_gate, w_proj):
        layers, rows_dev, emb_dim = ple_tables.shape
        me = lax.axis_index("emb")
        quarter = me % GROUP
        y_pos, z_pos = (me // Y) % 2, (me // Z) % 2
        cap_rows = tok_ids.shape[0] // CAP_DIV
        owner_dev = tok_ids // rows_dev
        local_row = tok_ids - owner_dev * rows_dev
        owner_hot = (owner_dev[:, None] == jnp.arange(shards, dtype=jnp.int32)[None, :]).astype(jnp.int32)
        slot_rank = jnp.sum((jnp.cumsum(owner_hot, axis=0) - owner_hot) * owner_hot, axis=1)
        dest_slot = owner_dev * cap_rows + slot_rank
        req_send = jnp.zeros((shards * cap_rows,), jnp.int32).at[dest_slot].set(local_row)
        req_recv = lax.all_to_all(req_send, "emb", 0, 0, tiled=True)
        sync = lax.optimization_barrier
        blocks = shards // GROUP

        def group(arr):
            twin = swap(arr, X)
            pair = jnp.concatenate([arr, twin], axis=-2)
            twin = swap(pair, CORE)
            return jnp.concatenate([pair, twin], axis=-2)

        last = layers - 1
        x_cur = x_in
        saved_list, rows_list, acts_list = [], [], []
        o_last = group(d_out)
        for layer in range(layers):
            served = jnp.take(ple_tables[layer], req_recv, axis=0)
            returned = lax.all_to_all(served, "emb", 0, 0, tiled=True)
            emb_rows = jnp.take(returned, dest_slot, axis=0)
            x_cur, saved = layer_fwd(x_cur, w_up[layer], w_down[layer], w_gate[layer], w_proj[layer], emb_rows)
            saved_list.append(saved)
            rows_list.append(emb_rows)
            acts_list.append(jnp.stack([saved[2], emb_rows]))
            if layer == 0:
                x_cur, o_last = sync((x_cur, o_last))
        x_out, acts_list = sync((x_cur, acts_list))

        def side_cols(arr):
            wide = arr.shape[-1]
            cut = arr.reshape(arr.shape[:-1] + (blocks, GROUP, wide // (blocks * GROUP)))
            pick = (jnp.arange(GROUP) == quarter)[:, None]
            return jnp.sum(jnp.where(pick, cut, 0), axis=-2).reshape(arr.shape[:-1] + (wide // GROUP,))

        def dx_step(layer, d_x):
            g_out = d_x.astype(jnp.bfloat16)
            d_x, d_rows = layer_bwd(d_x, g_out, saved_list[layer], rows_list[layer], w_up[layer], w_down[layer], w_gate[layer], w_proj[layer], layer > 0)
            return d_x, jnp.zeros((shards * cap_rows, emb_dim), jnp.float32).at[dest_slot].set(d_rows)

        def grads_head(layer, ue, o_rows):
            u_rows, e_part = ue[0], side_cols(ue[1])
            h_pre = dot32("nd,df->nf", u_rows, up_q[layer]).astype(jnp.bfloat16)
            z_pre = dot32("nd,de->ne", u_rows, gate_q[layer]).astype(jnp.bfloat16)
            d_act = dot32("nd,fd->nf", o_rows, down_q[layer]).astype(jnp.bfloat16)
            d_mix = dot32("nd,ed->ne", o_rows, proj_q[layer]).astype(jnp.bfloat16)
            act = gelu_tanh(h_pre.astype(jnp.float32)).astype(jnp.bfloat16)
            gate = gelu_tanh(z_pre.astype(jnp.float32)).astype(jnp.bfloat16)
            mix = (gate.astype(jnp.float32) * e_part.astype(jnp.float32)).astype(jnp.bfloat16)
            d_hid = gelu_back(h_pre, d_act).astype(jnp.bfloat16)
            d_gate = (e_part.astype(jnp.float32) * d_mix.astype(jnp.float32)).astype(jnp.bfloat16)
            d_pre = gelu_back(z_pre, d_gate).astype(jnp.bfloat16)
            return u_rows, o_rows, d_hid, d_pre, act, mix

        def grads_tail(u_rows, o_rows, d_hid, d_pre, act, mix):
            grads = [dot32("nf,nd->fd", lhs, rhs) for lhs, rhs in ((d_hid, u_rows), (d_pre, u_rows), (act, o_rows), (mix, o_rows))]
            return [g.reshape(2, 2, -1, g.shape[1]) for g in grads]

        def take(arrs, positions, axes):
            return [lax.dynamic_index_in_dim(arr, pos, axis=ax, keepdims=False) for arr, pos, ax in zip(arrs, positions, axes)]

        def sum_with(mine, sent, bits):
            return [own + swap(arr, bit) for own, arr, bit in zip(mine, sent, bits)]

        outs = blank([w_up.shape, w_gate.shape, w_down.shape, w_proj.shape, ple_tables.shape])
        col_outs, row_outs, table_out = (outs[0], outs[1]), (outs[2], outs[3]), outs[4]
        up_q, down_q, proj_q = weight_slices(quarter[None], w_up, w_gate, w_down, w_proj, blocks)
        gate_q = side_cols(w_gate)
        d_x = d_out.astype(jnp.float32)
        ue_last = group(acts_list[last])
        d_x, slots = dx_step(last, d_x)
        d_x, slots, ue_last, o_last = sync((d_x, slots, ue_last, o_last))
        recv = lax.all_to_all(slots, "emb", 0, 0, tiled=True)
        grads = grads_tail(*grads_head(last, ue_last, o_last))
        gathered = {}
        way1, way2 = (Y, Y, Z, Z), (Z, Z, Y, Y)
        pos1, pos2 = (y_pos, y_pos, z_pos, z_pos), (z_pos, z_pos, y_pos, y_pos)
        not1, not2 = [1 - p for p in pos1], [1 - p for p in pos2]
        for layer in reversed(range(layers)):
            sent = take(grads, not1, (1, 1, 0, 0))
            sent, grads, d_x = sync((sent, grads, d_x))
            sums = sum_with(take(grads, pos1, (1, 1, 0, 0)), sent, way1)
            if layer > 0:
                o_next = group(d_x.astype(jnp.bfloat16))
                ue_next = group(acts_list[layer - 1])
                d_x, slots = dx_step(layer - 1, d_x)
                sums, d_x, slots, o_next, ue_next, recv = sync((sums, d_x, slots, o_next, ue_next, recv))
            else:
                sums, recv = sync((sums, recv))
            sent = take(sums, not2, (0, 0, 0, 0))
            sent, sums = sync((sent, sums))
            sums = sum_with(take(sums, pos2, (0, 0, 0, 0)), sent, way2)
            table = jax.ops.segment_sum(recv, req_recv, num_segments=rows_dev)
            table_out = place_table(layer, table, table_out)
            if layer > 0:
                recv = lax.all_to_all(slots, "emb", 0, 0, tiled=True)
                head = grads_head(layer - 1, ue_next, o_next)
                sums, head, table_out = sync((sums, head, table_out))
            else:
                sums = sync(sums)
            cols_piece = jnp.concatenate(sums[:2], axis=0)
            rows_piece = jnp.concatenate(sums[2:], axis=0)
            if layer + 2 in gathered:
                ready = gathered.pop(layer + 2)
                col_outs = place_cols(layer + 2, ready[0], *col_outs)
                row_outs = place_rows(layer + 2, ready[1], *row_outs)
            if layer > 0:
                grads = grads_tail(*head)
            gathered[layer] = (lax.all_gather(cols_piece, "emb"), lax.all_gather(rows_piece, "emb"))
        for layer in sorted(gathered, reverse=True):
            cols_all, rows_all = gathered[layer]
            col_outs = place_cols(layer, cols_all, *col_outs)
            row_outs = place_rows(layer, rows_all, *row_outs)
        return (x_out, table_out, col_outs[0], row_outs[0], col_outs[1], row_outs[1])

    return jax.shard_map(
        device_step,
        mesh=mesh,
        in_specs=(P("emb"), P("emb", None), P("emb", None), P(None, "emb", None), P(), P(), P(), P()),
        out_specs=(P("emb", None), P(None, "emb", None), P(), P(), P(), P()),
        check_vma=False,
    )
```

```python
import jax
import jax.numpy as jnp
from jax import lax
from jax.experimental import pallas as pl
from jax.experimental.pallas import tpu as pltpu
from jax.sharding import PartitionSpec as P


EPS = 1e-6
CAP_DIV = 4
TIER_DIV = 4
CORE, X, Y, Z = 1, 2, 4, 8
GROUP = 4


def gelu_tanh(pre_act):
    return jax.nn.gelu(pre_act, approximate=True)


def gelu_back(pre_act, grad_out):
    _, pull_back = jax.vjp(gelu_tanh, pre_act.astype(jnp.float32))
    return pull_back(grad_out.astype(jnp.float32))[0]


def dot32(spec, a, b):
    return jnp.einsum(spec, a, b, preferred_element_type=jnp.float32)


def layer_fwd(x_cur, up_mat, down_mat, gate_mat, proj_mat, emb_rows):
    x_wide = x_cur.astype(jnp.float32)
    inv_rms = lax.rsqrt(jnp.mean(x_wide * x_wide, axis=-1, keepdims=True) + EPS)
    normed = (x_wide * inv_rms).astype(jnp.bfloat16)
    hidden = dot32("nd,df->nf", normed, up_mat).astype(jnp.bfloat16)
    act_out = gelu_tanh(hidden.astype(jnp.float32)).astype(jnp.bfloat16)
    mlp_out = dot32("nf,fd->nd", act_out, down_mat).astype(jnp.bfloat16)
    gate_pre = dot32("nd,de->ne", normed, gate_mat).astype(jnp.bfloat16)
    gate_act = gelu_tanh(gate_pre.astype(jnp.float32)).astype(jnp.bfloat16)
    mix_rows = (gate_act.astype(jnp.float32) * emb_rows.astype(jnp.float32)).astype(jnp.bfloat16)
    ple_out = dot32("ne,ed->nd", mix_rows, proj_mat).astype(jnp.bfloat16)
    x_next = (x_wide + mlp_out.astype(jnp.float32) + ple_out.astype(jnp.float32)).astype(jnp.bfloat16)
    return x_next, (x_wide, inv_rms, normed, hidden, gate_pre, gate_act)


def layer_bwd(d_x, g_out, saved, emb_rows, up_mat, down_mat, gate_mat, proj_mat, need_dx):
    x_wide, inv_rms, _, hidden, gate_pre, gate_act = saved
    d_mix = dot32("nd,ed->ne", g_out, proj_mat).astype(jnp.bfloat16)
    d_rows = gate_act.astype(jnp.float32) * d_mix.astype(jnp.float32)
    if not need_dx:
        return None, d_rows
    d_act = dot32("nd,fd->nf", g_out, down_mat).astype(jnp.bfloat16)
    d_hidden = gelu_back(hidden, d_act).astype(jnp.bfloat16)
    d_gate_act = (emb_rows.astype(jnp.float32) * d_mix.astype(jnp.float32)).astype(jnp.bfloat16)
    d_gate_pre = gelu_back(gate_pre, d_gate_act).astype(jnp.bfloat16)
    d_norm = dot32("nf,df->nd", d_hidden, up_mat) + dot32("ne,de->nd", d_gate_pre, gate_mat)
    d_x_new = d_x + inv_rms * d_norm - inv_rms ** 3 * x_wide * jnp.mean(d_norm * x_wide, axis=-1, keepdims=True)
    return d_x_new, d_rows


def cost(nbytes):
    return pl.CostEstimate(flops=int(nbytes), bytes_accessed=int(nbytes), transcendentals=0)


def weight_slices(quarter, w_up, w_gate, w_down, w_proj, blocks):
    layers, dim, hid = w_up.shape
    emb = w_gate.shape[2]
    hb, eb = hid // (GROUP * blocks), emb // (GROUP * blocks)

    def body(q_ref, up_ref, down_ref, proj_ref, up_out, down_out, proj_out):
        up_out[...] = up_ref[...]
        down_out[...] = down_ref[...]
        proj_out[...] = proj_ref[...]

    return pl.pallas_call(
        body,
        grid_spec=pltpu.PrefetchScalarGridSpec(
            num_scalar_prefetch=1,
            grid=(layers, blocks),
            in_specs=[
                pl.BlockSpec((1, dim, hb), lambda l, j, q: (l, 0, GROUP * j + q[0])),
                pl.BlockSpec((1, hb, dim), lambda l, j, q: (l, GROUP * j + q[0], 0)),
                pl.BlockSpec((1, eb, dim), lambda l, j, q: (l, GROUP * j + q[0], 0)),
            ],
            out_specs=[
                pl.BlockSpec((1, dim, hb), lambda l, j, q: (l, 0, j)),
                pl.BlockSpec((1, hb, dim), lambda l, j, q: (l, j, 0)),
                pl.BlockSpec((1, eb, dim), lambda l, j, q: (l, j, 0)),
            ],
        ),
        out_shape=[
            jax.ShapeDtypeStruct((layers, dim, hid // GROUP), w_up.dtype),
            jax.ShapeDtypeStruct((layers, hid // GROUP, dim), w_up.dtype),
            jax.ShapeDtypeStruct((layers, emb // GROUP, dim), w_up.dtype),
        ],
        cost_estimate=cost(4 * layers * dim * (2 * hid + emb) // GROUP),
        name="weight_slices",
    )(quarter, w_up, w_down, w_proj)


def blank(shapes):
    return pl.pallas_call(
        lambda *refs: None,
        out_shape=[jax.ShapeDtypeStruct(shape, jnp.float32) for shape in shapes],
        out_specs=[pl.BlockSpec(memory_space=pl.ANY)] * len(shapes),
        name="blank",
    )()


def place_cols(layer, buf, out_main, out_side):
    n, rows, dim = buf.shape
    hb = out_main.shape[2] // n
    eb = rows - hb
    at_once = max(1, 128 // eb)

    def body(buf_ref, main_in, side_in, main_ref, side_ref):
        for j in range(at_once):
            main_ref[0, :, j * hb:(j + 1) * hb] = buf_ref[j, :hb].T
        side = jnp.concatenate([buf_ref[j, hb:] for j in range(at_once)], axis=0)
        side_ref[0] = side.T

    return pl.pallas_call(
        body,
        grid=(n // at_once,),
        in_specs=[
            pl.BlockSpec((at_once, rows, dim), lambda j: (j, 0, 0)),
            pl.BlockSpec(memory_space=pl.ANY),
            pl.BlockSpec(memory_space=pl.ANY),
        ],
        out_specs=[
            pl.BlockSpec((1, dim, at_once * hb), lambda j: (layer, 0, j)),
            pl.BlockSpec((1, dim, at_once * eb), lambda j: (layer, 0, j)),
        ],
        out_shape=[
            jax.ShapeDtypeStruct(out_main.shape, out_main.dtype),
            jax.ShapeDtypeStruct(out_side.shape, out_side.dtype),
        ],
        input_output_aliases={1: 0, 2: 1},
        cost_estimate=cost(8 * n * rows * dim),
        name="place_cols",
    )(buf, out_main, out_side)


def place_rows(layer, buf, out_main, out_side):
    n, rows, dim = buf.shape
    hb = out_main.shape[1] // n
    eb = rows - hb
    at_once = 2

    def body(buf_ref, main_in, side_in, main_ref, side_ref):
        for j in range(at_once):
            main_ref[0, j * hb:(j + 1) * hb] = buf_ref[j, :hb]
            side_ref[0, j * eb:(j + 1) * eb] = buf_ref[j, hb:]

    return pl.pallas_call(
        body,
        grid=(n // at_once,),
        in_specs=[
            pl.BlockSpec((at_once, rows, dim), lambda j: (j, 0, 0)),
            pl.BlockSpec(memory_space=pl.ANY),
            pl.BlockSpec(memory_space=pl.ANY),
        ],
        out_specs=[
            pl.BlockSpec((1, at_once * hb, dim), lambda j: (layer, j, 0)),
            pl.BlockSpec((1, at_once * eb, dim), lambda j: (layer, j, 0)),
        ],
        out_shape=[
            jax.ShapeDtypeStruct(out_main.shape, out_main.dtype),
            jax.ShapeDtypeStruct(out_side.shape, out_side.dtype),
        ],
        input_output_aliases={1: 0, 2: 1},
        cost_estimate=cost(8 * n * rows * dim),
        name="place_rows",
    )(buf, out_main, out_side)


def place_table(layer, table, out):
    rows, dim = table.shape
    steps = 3 if rows % 24 == 0 else 1

    def body(table_ref, out_in, out_ref):
        out_ref[0] = table_ref[...]

    return pl.pallas_call(
        body,
        grid=(steps,),
        in_specs=[
            pl.BlockSpec((rows // steps, dim), lambda j: (j, 0)),
            pl.BlockSpec(memory_space=pl.ANY),
        ],
        out_specs=pl.BlockSpec((1, rows // steps, dim), lambda j: (layer, j, 0)),
        out_shape=jax.ShapeDtypeStruct(out.shape, out.dtype),
        input_output_aliases={1: 0},
        cost_estimate=cost(8 * rows * dim),
        name="place_table",
    )(table, out)


def solution(mesh):
    shards = mesh.shape["emb"]

    def swap(arr, axis_bit):
        return lax.ppermute(arr, "emb", [(dev, dev ^ axis_bit) for dev in range(shards)])

    def device_step(tok_ids, x_in, d_out, ple_tables, w_up, w_down, w_gate, w_proj):
        layers, rows_dev, emb_dim = ple_tables.shape
        me = lax.axis_index("emb")
        quarter = me % GROUP
        y_pos, z_pos = (me // Y) % 2, (me // Z) % 2
        cap_rows = tok_ids.shape[0] // CAP_DIV
        owner_dev = tok_ids // rows_dev
        local_row = tok_ids - owner_dev * rows_dev
        owner_hot = (owner_dev[:, None] == jnp.arange(shards, dtype=jnp.int32)[None, :]).astype(jnp.int32)
        slot_rank = jnp.sum((jnp.cumsum(owner_hot, axis=0) - owner_hot) * owner_hot, axis=1)
        dest_slot = owner_dev * cap_rows + slot_rank
        req_send = jnp.zeros((shards * cap_rows,), jnp.int32).at[dest_slot].set(local_row)
        req_recv = lax.all_to_all(req_send, "emb", 0, 0, tiled=True)
        tier_rows = cap_rows // TIER_DIV
        spilled = slot_rank >= tier_rows
        spill_rank = jnp.cumsum(spilled.astype(jnp.int32)) - 1
        tier_slot = jnp.where(spilled, shards * tier_rows + spill_rank, owner_dev * tier_rows + slot_rank)
        spill_ids = jnp.full((shards * tier_rows + cap_rows,), -1, jnp.int32).at[tier_slot].set(tok_ids)[shards * tier_rows:]
        spill_info = lax.all_gather(jnp.stack([spill_ids, jnp.full((cap_rows,), 1, jnp.int32) * (spill_rank[-1] + 1)]), "emb")
        req_recv, spill_info = lax.optimization_barrier((req_recv, spill_info))
        fits = jnp.max(spill_info[:, 1]) <= cap_rows
        spill_row = spill_info[:, 0].reshape(-1) - me * rows_dev
        spill_row = jnp.where((spill_row >= 0) & (spill_row < rows_dev), spill_row, rows_dev)
        sync = lax.optimization_barrier
        blocks = shards // GROUP

        def group(arr):
            twin = swap(arr, X)
            pair = jnp.concatenate([arr, twin], axis=-2)
            twin = swap(pair, CORE)
            return jnp.concatenate([pair, twin], axis=-2)

        last = layers - 1
        x_cur = x_in
        saved_list, rows_list, acts_list = [], [], []
        o_last = group(d_out)
        for layer in range(layers):
            served = jnp.take(ple_tables[layer], req_recv, axis=0)
            returned = lax.all_to_all(served, "emb", 0, 0, tiled=True)
            emb_rows = jnp.take(returned, dest_slot, axis=0)
            x_cur, saved = layer_fwd(x_cur, w_up[layer], w_down[layer], w_gate[layer], w_proj[layer], emb_rows)
            saved_list.append(saved)
            rows_list.append(emb_rows)
            acts_list.append(jnp.stack([saved[2], emb_rows]))
            if layer == 0:
                x_cur, o_last = sync((x_cur, o_last))
        x_out, acts_list = sync((x_cur, acts_list))

        def side_cols(arr):
            wide = arr.shape[-1]
            cut = arr.reshape(arr.shape[:-1] + (blocks, GROUP, wide // (blocks * GROUP)))
            pick = (jnp.arange(GROUP) == quarter)[:, None]
            return jnp.sum(jnp.where(pick, cut, 0), axis=-2).reshape(arr.shape[:-1] + (wide // GROUP,))

        def grads_head(layer, ue, o_rows):
            u_rows, e_part = ue[0], side_cols(ue[1])
            h_pre = dot32("nd,df->nf", u_rows, up_q[layer]).astype(jnp.bfloat16)
            z_pre = dot32("nd,de->ne", u_rows, gate_q[layer]).astype(jnp.bfloat16)
            d_act = dot32("nd,fd->nf", o_rows, down_q[layer]).astype(jnp.bfloat16)
            d_mix = dot32("nd,ed->ne", o_rows, proj_q[layer]).astype(jnp.bfloat16)
            act = gelu_tanh(h_pre.astype(jnp.float32)).astype(jnp.bfloat16)
            gate = gelu_tanh(z_pre.astype(jnp.float32)).astype(jnp.bfloat16)
            mix = (gate.astype(jnp.float32) * e_part.astype(jnp.float32)).astype(jnp.bfloat16)
            d_hid = gelu_back(h_pre, d_act).astype(jnp.bfloat16)
            d_gate = (e_part.astype(jnp.float32) * d_mix.astype(jnp.float32)).astype(jnp.bfloat16)
            d_pre = gelu_back(z_pre, d_gate).astype(jnp.bfloat16)
            return u_rows, o_rows, d_hid, d_pre, act, mix

        def grads_tail(u_rows, o_rows, d_hid, d_pre, act, mix):
            grads = [dot32("nf,nd->fd", lhs, rhs) for lhs, rhs in ((d_hid, u_rows), (d_pre, u_rows), (act, o_rows), (mix, o_rows))]
            return [g.reshape(2, 2, -1, g.shape[1]) for g in grads]

        def take(arrs, positions, axes):
            return [lax.dynamic_index_in_dim(arr, pos, axis=ax, keepdims=False) for arr, pos, ax in zip(arrs, positions, axes)]

        def sum_with(mine, sent, bits):
            return [own + swap(arr, bit) for own, arr, bit in zip(mine, sent, bits)]

        up_q, down_q, proj_q = weight_slices(quarter[None], w_up, w_gate, w_down, w_proj, blocks)
        gate_q = side_cols(w_gate)

        def backward(tiered):
            if tiered:
                slot_of, n_slots = tier_slot, shards * tier_rows + cap_rows
                base_row = req_recv.reshape(shards, cap_rows)[:, :tier_rows].reshape(-1)
                row_of = jnp.concatenate([base_row, spill_row])
            else:
                slot_of, n_slots, row_of = dest_slot, shards * cap_rows, req_recv

            def to_slots(d_rows):
                return jnp.zeros((n_slots, emb_dim), jnp.float32).at[slot_of].set(d_rows)

            def exchange(slots):
                if not tiered:
                    return (lax.all_to_all(slots, "emb", 0, 0, tiled=True),)
                cut = shards * tier_rows
                near = lax.all_to_all(slots[:cut], "emb", 0, 0, tiled=True)
                return near, lax.all_gather(slots[cut:], "emb", tiled=True)

            def add_rows(parts):
                return jax.ops.segment_sum(jnp.concatenate(parts, axis=0), row_of, num_segments=rows_dev)

            def dx_step(layer, d_x):
                g_out = d_x.astype(jnp.bfloat16)
                d_x, d_rows = layer_bwd(d_x, g_out, saved_list[layer], rows_list[layer], w_up[layer], w_down[layer], w_gate[layer], w_proj[layer], layer > 0)
                return d_x, to_slots(d_rows)

            outs = blank([w_up.shape, w_gate.shape, w_down.shape, w_proj.shape, ple_tables.shape])
            col_outs, row_outs, table_out = (outs[0], outs[1]), (outs[2], outs[3]), outs[4]
            d_x = d_out.astype(jnp.float32)
            ue_last = group(acts_list[last])
            d_x, slots = dx_step(last, d_x)
            d_x, slots, ue_last, o_first = sync((d_x, slots, ue_last, o_last))
            arrived = {last: exchange(slots)}
            grads = grads_tail(*grads_head(last, ue_last, o_first))
            gathered = {}
            way1, way2 = (Y, Y, Z, Z), (Z, Z, Y, Y)
            pos1, pos2 = (y_pos, y_pos, z_pos, z_pos), (z_pos, z_pos, y_pos, y_pos)
            not1, not2 = [1 - p for p in pos1], [1 - p for p in pos2]
            for layer in reversed(range(layers)):
                sent = take(grads, not1, (1, 1, 0, 0))
                sent, grads, d_x = sync((sent, grads, d_x))
                sums = sum_with(take(grads, pos1, (1, 1, 0, 0)), sent, way1)
                if layer > 0:
                    o_next = group(d_x.astype(jnp.bfloat16))
                    ue_next = group(acts_list[layer - 1])
                    d_x, slots = dx_step(layer - 1, d_x)
                    sums, d_x, slots, o_next, ue_next, table_out = sync((sums, d_x, slots, o_next, ue_next, table_out))
                else:
                    sums = sync(sums)
                sent = take(sums, not2, (0, 0, 0, 0))
                sent, sums = sync((sent, sums))
                sums = sum_with(take(sums, pos2, (0, 0, 0, 0)), sent, way2)
                if layer > 0:
                    arrived[layer - 1] = exchange(slots)
                    head = grads_head(layer - 1, ue_next, o_next)
                    sums, head, arrived[layer], table_out = sync((sums, head, arrived[layer], table_out))
                else:
                    sums, arrived[layer] = sync((sums, arrived[layer]))
                table_out = place_table(layer, add_rows(arrived[layer]), table_out)
                cols_piece = jnp.concatenate(sums[:2], axis=0)
                rows_piece = jnp.concatenate(sums[2:], axis=0)
                if layer + 2 in gathered:
                    ready = gathered.pop(layer + 2)
                    col_outs = place_cols(layer + 2, ready[0], *col_outs)
                    row_outs = place_rows(layer + 2, ready[1], *row_outs)
                if layer > 0:
                    grads = grads_tail(*head)
                gathered[layer] = (lax.all_gather(cols_piece, "emb"), lax.all_gather(rows_piece, "emb"))
            for layer in sorted(gathered, reverse=True):
                cols_all, rows_all = gathered[layer]
                col_outs = place_cols(layer, cols_all, *col_outs)
                row_outs = place_rows(layer, rows_all, *row_outs)
            return (table_out, col_outs[0], row_outs[0], col_outs[1], row_outs[1])

        return (x_out,) + lax.cond(fits, lambda: backward(True), lambda: backward(False))

    return jax.shard_map(
        device_step,
        mesh=mesh,
        in_specs=(P("emb"), P("emb", None), P("emb", None), P(None, "emb", None), P(), P(), P(), P()),
        out_specs=(P("emb", None), P(None, "emb", None), P(), P(), P(), P()),
        check_vma=False,
    )
```
